256 devices in a mesh: row: 8 (over z), col: 8 (over y, core), depth: 4 (over x).
Axes of the slice: x: 4, y: 4, z: 8, core: 2. Of those that a mesh axis runs over, the one named last changes fastest.
Arguments:
- a21_leaf: float32 [4, 4096, 2048], P('depth', 'row', 'col'), may hold values from -1.2 to 1.2
- a12_leaf: float32 [4, 2048, 4096], P('depth', 'row', 'col'), may hold values from -1.2 to 1.2
- uinv_leaf: float32 [4, 2048, 2048], P('depth', None, 'col'), may hold values from -0.2 to 1.5, as said below
- linv_leaf: float32 [4, 2048, 2048], P('depth', 'row'), may hold values from -0.2 to 1.5, as said below
- live: int32 [4], P('depth'), may hold values from 16 to 32
- row_map: int32 [4, 32], P('depth', 'row'), may hold values from 0 to 63, as said below
- col_map: int32 [4, 32], P('depth', 'col'), may hold values from 0 to 63, as said below
- a22_anc: float32 [8192, 8192], P(('row', 'depth'), 'col'), may hold values from -6 to 6
- a21_anc: float32 [8192, 2048], P(('row', 'depth'), 'col'), may hold values from -1.2 to 1.2
- a12_anc: float32 [2048, 8192], P(('row', 'depth'), 'col'), may hold values from -1.2 to 1.2
- uinv_anc: float32 [2048, 2048], P(None, 'col'), may hold values from -0.2 to 1.5, as said below
- linv_anc: float32 [2048, 2048], P(('row', 'depth')), may hold values from -0.2 to 1.5, as said below
Outputs:
- leaf_lower: float32 [4, 4096, 2048], P('depth', 'row', 'col')
- leaf_upper: float32 [4, 2048, 4096], P('depth', 'row', 'col')
- anc_lower: float32 [8192, 2048], P(('row', 'depth'), 'col')
- anc_upper: float32 [2048, 8192], P(('row', 'depth'), 'col')
- anc_schur: float32 [8192, 8192], P(('row', 'depth'), 'col')
The draws below stay inside these ranges and needn't reach their ends.
Inputs may be any that keep to these rules, and one draw needn't show every extreme that they name: `uinv_leaf`: upper triangular: zero below the diagonal, diagonal between 0.5 and 1.5. `linv_leaf`: lower triangular: zero above the diagonal, diagonal between 0.5 and 1.5. `uinv_anc`: upper triangular: zero below the diagonal, diagonal between 0.5 and 1.5. `linv_anc`: lower triangular: zero above the diagonal, diagonal between 0.5 and 1.5. `row_map`: within one replica the entries are distinct. Leaf block row i lies in the k-th of 8 equal ranges of leaf block rows, and its target lies in the k-th of 8 equal ranges of the 64 ancestor block rows. `col_map`: within one replica the entries are distinct. Leaf block column j lies in the k-th of 8 equal ranges of leaf block columns, and its target lies in the k-th of 8 equal ranges of the 64 ancestor block columns.
All inputs are finite; a program needn't handle non-finite values.
Results may differ from the reference program's by a relative error of at most 0.0001.
Values sent between devices are 32-bit elements; how exact they have to be, the bound alone decides.
No kernel may reach another device: no remote copies, remote signals or barrier semaphores. Data moves between devices by JAX's collectives and lax.ppermute only.
A program may use at most 128 MiB of HBM per device.

```python
from functools import partial
import jax
import jax.numpy as jnp
from jax import lax

NB = 128
WL = 2048
WA = 2048
R = 4096
RA = 8192
N_ROW = 8
N_COL = 8
N_DEPTH = 4


def triangle(subkey, order, upper):
    first, second = jax.random.split(subkey)
    spread = jnp.clip(jax.random.normal(first, (order, order), jnp.float32) * (0.5 / order ** 0.5), -0.2, 0.2)
    diagonal = jax.random.uniform(second, (order,), jnp.float32, 0.5, 1.5)
    if upper:
        strict = jnp.triu(spread, 1)
    else:
        strict = jnp.tril(spread, -1)
    return strict + jnp.diag(diagonal)


def draw_uinv_leaf(key, part):
    subkeys = jax.random.split(jax.random.fold_in(key, 11), N_DEPTH)
    return jax.vmap(partial(triangle, order=WL, upper=True))(subkeys)


def draw_linv_leaf(key, part):
    subkeys = jax.random.split(jax.random.fold_in(key, 12), N_DEPTH)
    return jax.vmap(partial(triangle, order=WL, upper=False))(subkeys)


def draw_uinv_anc(key, part):
    return triangle(jax.random.fold_in(key, 13), WA, True)


def draw_linv_anc(key, part):
    return triangle(jax.random.fold_in(key, 14), WA, False)


def pick_targets(subkey, per_leaf, per_anc):
    return jax.random.permutation(subkey, per_anc)[:per_leaf]


def owner_map(key, groups):
    per_leaf = R // (NB * groups)
    per_anc = RA // (NB * groups)
    subkeys = jax.random.split(key, N_DEPTH * groups)
    chosen = jax.vmap(partial(pick_targets, per_leaf=per_leaf, per_anc=per_anc))(subkeys)
    base = jnp.arange(N_DEPTH * groups) % groups * per_anc
    return (chosen + base[:, None]).reshape(N_DEPTH, groups * per_leaf).astype(jnp.int32)


def draw_row_map(key, part):
    return owner_map(jax.random.fold_in(key, 16), N_ROW)


def draw_col_map(key, part):
    return owner_map(jax.random.fold_in(key, 17), N_COL)


def place_ends(array, own_key, smallest, high):
    index_at = [jax.random.randint(jax.random.fold_in(own_key, axis), (), 0, length) for axis, length in enumerate(array.shape)]
    longest = array.shape.index(max(array.shape))
    beside = index_at[:longest] + [(index_at[longest] + 1) % array.shape[longest]] + index_at[longest + 1:]
    return array.at[tuple(index_at)].set(smallest).at[tuple(beside)].set(high)


def levels(own_key, extent, shards, least, top_value):
    loudness, own = 1.0, jax.random.fold_in(own_key, 6)
    for axis_at, parts in shards:
        draws = jnp.exp(jax.random.uniform(jax.random.fold_in(own, axis_at), (parts,), jnp.float32, least / len(shards), top_value / len(shards)))
        loudness = loudness * jnp.repeat(draws, extent[axis_at] // parts).reshape([-1 if axis == axis_at else 1 for axis in range(len(extent))])
    return loudness


def gaussian(stream_key, shape, scale, most, pieces=(), kind=jnp.bfloat16):
    drawn = scale * jax.random.normal(stream_key, shape, jnp.float32)
    if pieces:
        drawn = drawn * levels(stream_key, shape, pieces, -0.22, 0.18)
    return jnp.clip(drawn, -most, most).astype(kind)


def setup_inputs(seed: int = 0) -> dict:
    seeds = jax.random.split(jax.random.key(seed), 13)
    a21_leaf = gaussian(seeds[0], (N_DEPTH, R, WL), 0.18, 1.2, ((0, 4), (1, 8), (2, 8)), jnp.float32)
    a12_leaf = gaussian(seeds[1], (N_DEPTH, WL, R), 0.18, 1.2, ((0, 4), (1, 8), (2, 8)), jnp.float32)
    uinv_leaf = draw_uinv_leaf(jax.random.fold_in(seeds[12], 71), 0)
    linv_leaf = draw_linv_leaf(jax.random.fold_in(seeds[12], 71), 0)
    live = place_ends(jax.random.randint(seeds[4], (N_DEPTH,), R // NB // 2, R // NB + 1), jax.random.fold_in(seeds[4], 1), R // NB // 2, (R // NB + 1) - 1).astype(jnp.int32)
    row_map = draw_row_map(jax.random.fold_in(seeds[12], 71), 0)
    col_map = draw_col_map(jax.random.fold_in(seeds[12], 71), 0)
    a22_anc = gaussian(seeds[7], (RA, RA), 1.0, 6.0, ((0, 32), (1, 8)), jnp.float32)
    a21_anc = gaussian(seeds[8], (RA, WA), 0.18, 1.2, ((0, 32), (1, 8)), jnp.float32)
    a12_anc = gaussian(seeds[9], (WA, RA), 0.18, 1.2, ((0, 32), (1, 8)), jnp.float32)
    uinv_anc = draw_uinv_anc(jax.random.fold_in(seeds[12], 71), 0)
    linv_anc = draw_linv_anc(jax.random.fold_in(seeds[12], 71), 0)
    return {"a21_leaf": a21_leaf, "a12_leaf": a12_leaf, "uinv_leaf": uinv_leaf, "linv_leaf": linv_leaf, "live": live, "row_map": row_map, "col_map": col_map, "a22_anc": a22_anc, "a21_anc": a21_anc, "a12_anc": a12_anc, "uinv_anc": uinv_anc, "linv_anc": linv_anc}


def product(left, right):
    return jnp.dot(left, right, precision=lax.Precision.HIGHEST, preferred_element_type=jnp.float32)


def reference(a21_leaf, a12_leaf, uinv_leaf, linv_leaf, live, row_map, col_map, a22_anc, a21_anc, a12_anc, uinv_anc, linv_anc):
    positions = jnp.arange(R, dtype=jnp.int32)
    block_ids = (positions // NB).astype(jnp.int32)
    offsets = (positions % NB).astype(jnp.int32)
    update = jnp.zeros((RA, RA), jnp.float32)
    lowers = []
    uppers = []
    for depth in range(N_DEPTH):
        keep = (block_ids < live[depth]).astype(jnp.float32)
        lower = product(a21_leaf[depth], uinv_leaf[depth]) * keep[:, None]
        upper = product(linv_leaf[depth], a12_leaf[depth]) * keep[None, :]
        schur = -product(lower, upper)
        rows = (row_map[depth][block_ids] * NB + offsets).astype(jnp.int32)
        cols = (col_map[depth][block_ids] * NB + offsets).astype(jnp.int32)
        update = update.at[rows[:, None], cols[None, :]].add(schur)
        lowers.append(lower)
        uppers.append(upper)
    leaf_lower = jnp.stack(lowers)
    leaf_upper = jnp.stack(uppers)
    anc_lower = product(a21_anc, uinv_anc)
    anc_upper = product(linv_anc, a12_anc)
    anc_schur = a22_anc + update - product(anc_lower, anc_upper)
    return leaf_lower, leaf_upper, anc_lower, anc_upper, anc_schur
```

```python
import functools

import jax
import jax.numpy as jnp
from jax import lax
from jax.experimental import pallas as pl
from jax.experimental.pallas import tpu as pltpu
from jax.sharding import PartitionSpec as P

NB = 128
F32 = jnp.float32


def shift(block, axis, step):
    size = lax.axis_size(axis)
    return lax.ppermute(block, axis, [(i, (i + step) % size) for i in range(size)])


def swap_cores(block):
    return lax.ppermute(block, "col", [(i, i ^ 1) for i in range(lax.axis_size("col"))])


def gather_row(block):
    half = block.shape[0] // 2
    got = [(0, 0, block)]
    up = down = block
    steps = lax.axis_size("row") // 2
    for step in range(1, steps):
        up = shift(up, "row", 1)
        down = shift(down, "row", -1)
        got += [(step, 0, up), (-step, 0, down)]
    got += [(steps, 0, shift(up[:half], "row", 1)), (steps, half, shift(down[half:], "row", -1))]
    return got


def gather_col(block):
    half = block.shape[0] // 2
    up = shift(block, "col", 2)
    down = shift(block, "col", -2)
    mine = [(0, 0, block), (2, 0, down), (6, 0, up)]
    mine += [(4, 0, shift(up[:half], "col", 2)), (4, half, shift(down[half:], "col", -2))]
    return mine + [(place + 1, start, swap_cores(b)) for place, start, b in mine]


def exchange_depth(parts):
    size = len(parts)
    return [parts[0]] + [shift(parts[size - j], "depth", -j) for j in range(1, size)]


def sum_depth(parts):
    own, (one_top, one_bot), (two_top, two_bot), (three_top, three_bot) = parts
    from_back = shift(two_top, "depth", 1)
    from_front = shift(two_bot, "depth", -1)
    back_bot = shift(one_bot, "depth", 1)
    front_top = shift(three_top, "depth", -1)
    back_top = shift(one_top + from_back, "depth", 1)
    front_bot = shift(three_bot + from_front, "depth", -1)
    return own, back_top, back_bot, front_top, front_bot


def split(x):
    high = x.astype(jnp.bfloat16)
    return high, (x - high.astype(F32)).astype(jnp.bfloat16)


def dot3(left, right, dims=(((1,), (0,)), ((), ()))):
    (lh, ll), (rh, rl) = left, right
    dot = functools.partial(lax.dot_general, dimension_numbers=dims, preferred_element_type=F32)
    return dot(lh, rh) + (dot(lh, rl) + dot(ll, rh))


def copy_all(copies, sems):
    started = [pltpu.make_async_copy(src, dst, sems.at[i]) for i, (src, dst) in enumerate(copies)]
    for c in started:
        c.start()
    for c in started:
        c.wait()


def call(kernel, arrays, scalars, outs, scratch, copies, flops):
    any_spec = pl.BlockSpec(memory_space=pl.ANY)
    return pl.pallas_call(
        kernel,
        in_specs=[pl.BlockSpec(memory_space=pltpu.SMEM)] * len(scalars) + [any_spec] * len(arrays),
        out_specs=[pl.BlockSpec(memory_space=pltpu.VMEM)] * len(outs),
        out_shape=[jax.ShapeDtypeStruct(s, F32) for s in outs],
        scratch_shapes=[pltpu.VMEM(s, F32) for s in scratch] + [pltpu.SemaphoreType.DMA((copies,))],
        compiler_params=pltpu.CompilerParams(vmem_limit_bytes=56 * 2**20),
        cost_estimate=pl.CostEstimate(flops=flops, bytes_accessed=2**20, transcendentals=0),
    )(*scalars, *arrays)


def row_of(back, size):
    return lax.rem(lax.axis_index("row") + (size - back), size)


def place_of(column, chips):
    me = lax.axis_index("col")
    ahead = lax.rem(column // 2 - me // 2 + chips, chips)
    return ahead * 2 + lax.rem(column + me, 2)


def column_at(place, chips):
    me = lax.axis_index("col")
    return lax.rem(me // 2 + place // 2, chips) * 2 + lax.rem(me + place, 2)


def anc_upper_parts(got_linv, top):
    n_row = lax.axis_size("row")
    k, wide = top[0][2].shape
    m, kk = got_linv[0].shape
    n = len(got_linv)

    def kernel(*refs):
        linv = refs[:n]
        blocks = refs[n : n + len(top)]
        outs = refs[n + len(top) : -3]
        left, right, sems = refs[-3:]
        copies = [(ref, left.at[j]) for j, ref in enumerate(linv)]
        for (back, start, a), ref in zip(top, blocks):
            copies.append((ref, right.at[row_of(back, n_row), pl.ds(start, a.shape[0])]))
        copy_all(copies, sems)
        got = dot3(split(left[...].reshape(n * m, kk)), split(right[...].reshape(kk, wide)))
        outs[0][...] = got[:m]
        half = m // 2
        for i, out in enumerate(outs[1:]):
            out[...] = got[m + i * half : m + (i + 1) * half]

    outs = [(m, wide)] + [(m // 2, wide)] * (2 * (n - 1))
    res = call(
        kernel,
        [*got_linv, *[a for *_, a in top]],
        [],
        outs,
        [(n, m, kk), (n_row, k, wide)],
        n + len(top),
        2 * n * m * kk * wide,
    )
    return [res[0]] + [tuple(res[i : i + 2]) for i in range(1, len(res), 2)]


def finish_anc_upper(own, *halves):
    back_top, back_bot, front_top, front_bot = halves
    half = own.shape[0] // 2
    return jnp.concatenate(
        [own[:half] + back_top + front_top, own[half:] + back_bot + front_bot], axis=0
    )


def lower_panels(lefts, uinv_leaf, uinv_anc, live, rows_here, n_depth):
    n_col = lax.axis_size("col")
    chips = n_col // 2
    width = lefts[0][2].shape[1]
    tall = lefts[0][2].shape[0]
    anc_rows = tall - rows_here
    kd = width // n_depth

    def kernel(live_ref, ul, ua, *refs):
        blocks = refs[: len(lefts)]
        leaf_out, anc_out, *sends = refs[len(lefts) : -5]
        left, right_l, right_a, turned, sems = refs[-5:]
        copies = []
        for (place, start, a), ref in zip(lefts, blocks):
            copies.append(
                (ref, left.at[pl.ds(start, a.shape[0]), pl.ds(place * width, width)])
            )
        for place in range(n_col):
            at = column_at(place, chips) * width
            to = pl.ds(place * width, width)
            copies.append((ul.at[pl.ds(at, width)], right_l.at[to]))
            copies.append((ua.at[pl.ds(at, width)], right_a.at[to]))
        copy_all(copies, sems)
        leaf = dot3(split(left[:rows_here]), split(right_l[...]))
        rows = lax.axis_index("row") * rows_here + lax.broadcasted_iota(jnp.int32, leaf.shape, 0)
        leaf_out[...] = jnp.where(rows < live_ref[0] * NB, leaf, 0.0)
        anc = dot3(split(left[rows_here:]), split(right_a[...]))
        anc_out[...] = anc
        turned[...] = anc.T.reshape(n_depth, kd, anc_rows)
        me = lax.axis_index("depth")
        for j, out in enumerate(sends):
            out[...] = turned[lax.rem(me + j, n_depth)]

    res = call(
        kernel,
        [uinv_leaf, uinv_anc, *[a for *_, a in lefts]],
        [live],
        [(rows_here, width), (anc_rows, width)] + [(kd, anc_rows)] * n_depth,
        [
            (tall, n_col * width),
            (n_col * width, width),
            (n_col * width, width),
            (n_depth, kd, anc_rows),
        ],
        len(lefts) + 2 * n_col,
        2 * tall * n_col * width * width,
    )
    return res[0], res[1], res[2:]


def leaf_upper_panel(linv, top, live):
    n_row = lax.axis_size("row")
    k, wide = top[0][2].shape
    m = linv.shape[0]

    def kernel(live_ref, linv_ref, *refs):
        blocks = refs[: len(top)]
        out, left, right, sems = refs[len(top) :]
        copies = [(linv_ref, left)]
        for (back, start, a), ref in zip(top, blocks):
            copies.append((ref, right.at[row_of(back, n_row), pl.ds(start, a.shape[0])]))
        copy_all(copies, sems)
        got = dot3(split(left[...]), split(right[...].reshape(n_row * k, wide)))
        cols = lax.axis_index("col") * wide + lax.broadcasted_iota(jnp.int32, got.shape, 1)
        out[...] = jnp.where(cols < live_ref[0] * NB, got, 0.0)

    return call(
        kernel,
        [linv, *[a for *_, a in top]],
        [live],
        [(m, wide)],
        [(m, n_row * k), (n_row, k, wide)],
        1 + len(top),
        2 * m * n_row * k * wide,
    )[0]


def anc_product(lowers, uppers, rows_here, n_depth):
    n_row, n_col = lax.axis_size("row"), lax.axis_size("col")
    chips = n_col // 2
    kd, wide = uppers[0][2].shape
    tall, anc_rows = lowers[0][2].shape
    half = tall // 2

    def kernel(*refs):
        blocks = refs[: len(lowers)]
        ups = refs[len(lowers) : len(lowers) + len(uppers)]
        out, left, right, sems = refs[-4:]
        copies = []
        for (place, start, a), ref in zip(lowers, blocks):
            if start + a.shape[0] <= rows_here:
                continue
            for j in range(n_depth):
                first = rows_here + j * kd - start
                if first < 0:
                    continue
                copies.append((ref.at[pl.ds(first, kd)], left.at[j, pl.ds(place * kd, kd)]))
        for (back, start, a), ref in zip(uppers, ups):
            place = place_of(row_of(back, n_row), chips)
            copies.append((ref, right.at[place, pl.ds(start, a.shape[0])]))
        copy_all(copies, sems)
        upper = split(right[...].reshape(n_row * kd, wide))
        for j in range(n_depth):
            turned = split(left[j].T)
            out[pl.ds(j * anc_rows, anc_rows)] = dot3(turned, upper)

    assert half <= rows_here
    return call(
        kernel,
        [*[a for *_, a in lowers], *[a for *_, a in uppers]],
        [],
        [(n_depth * anc_rows, wide)],
        [(n_depth, n_col * kd, anc_rows), (n_row, kd, wide)],
        n_depth * len(lowers) + len(uppers),
        2 * n_depth * anc_rows * n_row * kd * wide,
    )[0]


def front_parts(lowers, uppers, product, row_map, col_map, rows_here, n_depth):
    n_row, n_col = lax.axis_size("row"), lax.axis_size("col")
    chips = n_col // 2
    nb = NB
    width = lowers[0][2].shape[1]
    k, cols_here = uppers[0][2].shape
    front, wide = product.shape
    owner_rows = front // n_depth
    per_owner = owner_rows // nb
    leaf_rows, leaf_cols = rows_here // nb, cols_here // nb

    def kernel(rm, cm, prod, *refs):
        blocks = refs[: len(lowers)]
        ups = refs[len(lowers) : len(lowers) + len(uppers)]
        outs = refs[len(lowers) + len(uppers) : -4]
        left, right, acc, sems = refs[-4:]
        copies = [(prod, acc)]
        for (place, start, a), ref in zip(lowers, blocks):
            n = min(a.shape[0], rows_here - start)
            if n > 0:
                copies.append(
                    (ref.at[pl.ds(0, n)], left.at[pl.ds(start, n), pl.ds(place * width, width)])
                )
        for (back, start, a), ref in zip(uppers, ups):
            place = place_of(row_of(back, n_row), chips)
            copies.append((ref, right.at[place, pl.ds(start, a.shape[0])]))
        copy_all(copies, sems)
        leaf = dot3(split(left[...]), split(right[...].reshape(n_row * k, cols_here)))
        first_row = lax.axis_index("row") * (front // nb)
        first_col = lax.axis_index("col") * (wide // nb)
        me = lax.axis_index("depth")
        for i in range(leaf_rows):
            at = rm[0, i] - first_row
            ahead = lax.rem(at // per_owner - me + n_depth, n_depth)
            row = (ahead * per_owner + lax.rem(at, per_owner)) * nb
            rows = pl.ds(pl.multiple_of(row, nb), nb)
            for j in range(leaf_cols):
                cols = pl.ds(pl.multiple_of((cm[0, j] - first_col) * nb, nb), nb)
                acc[rows, cols] += leaf[i * nb : (i + 1) * nb, j * nb : (j + 1) * nb]
        outs[0][...] = acc[:owner_rows]
        half = owner_rows // 2
        for i, out in enumerate(outs[1:]):
            out[...] = acc[pl.ds(owner_rows + i * half, half)]

    res = call(
        kernel,
        [product, *[a for *_, a in lowers], *[a for *_, a in uppers]],
        [row_map, col_map],
        [(owner_rows, wide)] + [(owner_rows // 2, wide)] * (2 * (n_depth - 1)),
        [(rows_here, n_col * width), (n_row, k, cols_here), (front, wide)],
        1 + len(lowers) + len(uppers),
        2 * rows_here * n_row * k * cols_here,
    )
    return [res[0]] + [tuple(res[i : i + 2]) for i in range(1, len(res), 2)]


def shards(
    a21_leaf,
    a12_leaf,
    uinv_leaf,
    linv_leaf,
    live,
    row_map,
    col_map,
    a22_anc,
    a21_anc,
    a12_anc,
    uinv_anc,
    linv_anc,
):
    n_row, n_depth = lax.axis_size("row"), lax.axis_size("depth")
    depth = lax.axis_index("depth")
    panel_left, panel_top = a21_leaf[0], a12_leaf[0]
    rows_here = panel_left.shape[0]

    anc_top = gather_row(a12_anc)
    leaf_top = gather_row(panel_top)
    k_here = a12_anc.shape[0]
    by_depth = linv_anc.reshape(k_here, n_row, n_depth, k_here).transpose(2, 0, 1, 3)
    by_depth = by_depth.reshape(n_depth, k_here, n_row * k_here)
    turned = [
        lax.dynamic_index_in_dim(by_depth, lax.rem(depth + j, n_depth), 0, keepdims=False)
        for j in range(n_depth)
    ]
    linv_got = exchange_depth(turned)
    lefts = gather_col(jnp.concatenate([panel_left, a21_anc], axis=0))

    anc_upper = finish_anc_upper(*sum_depth(anc_upper_parts(linv_got, anc_top)))
    leaf_lower, anc_lower, slices = lower_panels(
        lefts, uinv_leaf[0], uinv_anc, live, rows_here, n_depth
    )
    leaf_upper = leaf_upper_panel(linv_leaf[0], leaf_top, live)

    anc_uppers = gather_row(anc_upper)
    leaf_uppers = gather_row(leaf_upper)
    lowers = gather_col(jnp.concatenate([leaf_lower, *exchange_depth(slices)], axis=0))

    product = anc_product(lowers, anc_uppers, rows_here, n_depth)
    parts = front_parts(lowers, leaf_uppers, product, row_map, col_map, rows_here, n_depth)
    own, back_top, back_bot, front_top, front_bot = sum_depth(parts)
    half = own.shape[0] // 2
    total_top = own[:half] + back_top + front_top
    total_bot = own[half:] + back_bot + front_bot
    anc_schur = a22_anc - jnp.concatenate([total_top, total_bot], axis=0)
    return (leaf_lower[None], leaf_upper[None], anc_lower, anc_upper, anc_schur)


def solution(mesh):
    in_specs = (
        P("depth", "row", "col"),
        P("depth", "row", "col"),
        P("depth", None, "col"),
        P("depth", "row", None),
        P("depth"),
        P("depth", "row"),
        P("depth", "col"),
        P(("row", "depth"), "col"),
        P(("row", "depth"), "col"),
        P(("row", "depth"), "col"),
        P(None, "col"),
        P(("row", "depth"), None),
    )
    out_specs = (
        P("depth", "row", "col"),
        P("depth", "row", "col"),
        P(("row", "depth"), "col"),
        P(("row", "depth"), "col"),
        P(("row", "depth"), "col"),
    )
    return jax.shard_map(shards, mesh=mesh, in_specs=in_specs, out_specs=out_specs, check_vma=False)
```

```python
import functools

import jax
import jax.numpy as jnp
from jax import lax
from jax.experimental import pallas as pl
from jax.experimental.pallas import tpu as pltpu
from jax.sharding import PartitionSpec as P

NB = 128
F32 = jnp.float32
BF16 = jnp.bfloat16


def shift(block, axis, step):
    size = lax.axis_size(axis)
    return lax.ppermute(block, axis, [(i, (i + step) % size) for i in range(size)])


def swap_cores(block):
    return lax.ppermute(block, "col", [(i, i ^ 1) for i in range(lax.axis_size("col"))])


def gather_row(block, far):
    steps = lax.axis_size("row") // 2
    got = [(0, block)]
    for way, sign in (("u", 1), ("d", -1)):
        moving = block
        for step in range(1, steps + (way == far)):
            moving = shift(moving, "row", sign)
            got.append((sign * step, moving))
    return sorted(got, key=lambda item: abs(item[0]))


def gather_col(halves):
    n_col = lax.axis_size("col")
    copies = jnp.broadcast_to(halves, (n_col // 2, *halves.shape)).reshape(n_col, *halves.shape[1:])
    mine = lax.all_to_all(copies, "col", split_axis=0, concat_axis=0, tiled=True)
    return mine, swap_cores(mine)


def exchange_depth(parts):
    return lax.all_to_all(parts, "depth", split_axis=0, concat_axis=0, tiled=True)


def exchange_depth_rings(parts):
    size = len(parts)
    return [parts[0]] + [shift(parts[size - j], "depth", -j) for j in range(1, size)]


def sum_depth(parts):
    own, (one_top, one_bot), (two_top, two_bot), (three_top, three_bot) = parts
    from_back = shift(two_top, "depth", 1)
    from_front = shift(two_bot, "depth", -1)
    back_bot = shift(one_bot, "depth", 1)
    front_top = shift(three_top, "depth", -1)
    back_top = shift(one_top + from_back, "depth", 1)
    front_bot = shift(three_bot + from_front, "depth", -1)
    return own, back_top, back_bot, front_top, front_bot


def split(x):
    high = x.astype(BF16)
    return high, (x - high.astype(F32)).astype(BF16)


def dot3(left, right):
    (lh, ll), (rh, rl) = left, right
    dot = functools.partial(jnp.dot, preferred_element_type=F32)
    return dot(lh, rh) + (dot(lh, rl) + dot(ll, rh))


def start_all(copies, sems):
    started = [pltpu.make_async_copy(src, dst, sems.at[i]) for i, (src, dst) in enumerate(copies)]
    for c in started:
        c.start()
    return started


def copy_all(copies, sems):
    for c in start_all(copies, sems):
        c.wait()


def add_up(out, tiles, started, per_tile, left, right, fresh=True):
    for t in range(tiles):
        for c in started[t * per_tile : (t + 1) * per_tile]:
            c.wait()
        got = dot3(split(left(t)), split(right(t)))
        out[...] = got if fresh and t == 0 else out[...] + got


def call(kernel, arrays, scalars, outs, scratch, copies, flops):
    specs = [pl.BlockSpec(memory_space=pltpu.SMEM)] * len(scalars)
    specs += [pl.BlockSpec(memory_space=pl.ANY)] * len(arrays)
    return pl.pallas_call(
        kernel,
        in_specs=specs,
        out_specs=[pl.BlockSpec(memory_space=pltpu.VMEM)] * len(outs),
        out_shape=[jax.ShapeDtypeStruct(s, F32) for s in outs],
        scratch_shapes=[
            pltpu.VMEM(s, F32) if isinstance(s[0], int) else pltpu.VMEM(s[0], s[1]) for s in scratch
        ]
        + [pltpu.SemaphoreType.DMA((copies,))],
        compiler_params=pltpu.CompilerParams(vmem_limit_bytes=56 * 2**20),
        cost_estimate=pl.CostEstimate(flops=flops, bytes_accessed=2**20, transcendentals=0),
    )(*scalars, *arrays)


def row_of(back):
    size = lax.axis_size("row")
    return lax.rem(lax.axis_index("row") + (size - back), size)


def core_halves():
    mine = lax.rem(lax.axis_index("col"), 2)
    return mine, 1 - mine


def split_by_depth(linv, n_row, n_depth):
    k, wide = linv.shape
    kd = wide // (n_row * n_depth)

    def kernel(ref, *refs):
        outs, parts = refs[:n_depth], refs[-2]
        for q in range(n_depth):
            cols = [ref[:, (r * n_depth + q) * kd : (r * n_depth + q + 1) * kd] for r in range(n_row)]
            parts[q] = jnp.concatenate(cols, axis=1)
        me = lax.axis_index("depth")
        for j, out in enumerate(outs):
            out[...] = parts[lax.rem(me + j, n_depth)]

    vmem = pl.BlockSpec(memory_space=pltpu.VMEM)
    return pl.pallas_call(
        kernel,
        in_specs=[vmem],
        out_specs=[vmem] * n_depth,
        out_shape=[jax.ShapeDtypeStruct((k, n_row * kd), F32)] * n_depth,
        scratch_shapes=[pltpu.VMEM((n_depth, k, n_row * kd), F32), pltpu.SemaphoreType.DMA((1,))],
    )(linv)


def anc_upper_parts(got_linv, top):
    n_row = lax.axis_size("row")
    k, wide = top[0][1].shape
    n = len(got_linv)
    m, kk = got_linv[0].shape
    tiles = 2
    kt = kk // tiles

    def kernel(*refs):
        linv, blocks, outs = refs[:n], refs[n : n + len(top)], refs[n + len(top) : -4]
        left, right, acc, sems = refs[-4:]
        copies = []
        for j, ref in enumerate(linv):
            for t in range(tiles):
                copies.append((ref.at[:, pl.ds(t * kt, kt)], left.at[t, j]))
        for (back, _), ref in zip(top, blocks):
            copies.append((ref, right.at[row_of(back)]))
        copy_all(copies, sems)

        def step(t, _):
            rows = right[pl.ds(t * (n_row // tiles), n_row // tiles)].reshape(kt, wide)
            got = dot3(split(left[t].reshape(n * m, kt)), split(rows)).reshape(n, m, wide)
            acc[...] = jnp.where(t == 0, got, acc[...] + got)
            return 0

        lax.fori_loop(0, tiles, step, 0)
        for j, out in enumerate(outs):
            out[...] = acc[j]

    return call(
        kernel,
        [*got_linv, *[a for _, a in top]],
        [],
        [(m, wide)] * n,
        [(tiles, n, m, kt), (n_row, k, wide), (n, m, wide)],
        tiles * n + len(top),
        2 * n * m * kk * wide,
    )


def lower_panels(lefts, uinv_leaf, uinv_anc, live, rows_here, n_depth):
    n_col, tall, width = lefts[0].shape
    leaf_half = rows_here // 2
    anc_half = tall - leaf_half
    anc_rows = 2 * anc_half
    kd = width // n_depth

    def kernel(live_ref, ul, ua, mine, other, leaf_out, anc_out, turned, *scratch):
        left_l, left_a, right_l, right_a, sems = scratch
        copies = []
        for t in range(n_col):
            rows = pl.ds(t * width, width)
            copies += [(ul.at[rows], right_l.at[t]), (ua.at[rows], right_a.at[t])]
            for which, ref in zip(core_halves(), (mine, other)):
                copies += [
                    (ref.at[t, pl.ds(0, leaf_half)], left_l.at[t, which]),
                    (ref.at[t, pl.ds(leaf_half, anc_half)], left_a.at[t, which]),
                ]
        started = start_all(copies, sems)
        anc = lambda t: left_a[t].reshape(anc_rows, width)
        leaf = lambda t: left_l[t].reshape(rows_here, width)
        add_up(anc_out, n_col, started, 6, anc, lambda t: right_a[t])
        add_up(leaf_out, n_col, started, 0, leaf, lambda t: right_l[t])
        rows = lax.axis_index("row") * rows_here + lax.broadcasted_iota(jnp.int32, leaf_out.shape, 0)
        leaf_out[...] = jnp.where(rows < live_ref[0] * NB, leaf_out[...], 0.0)
        turned[...] = anc_out[...].T.reshape(n_depth, kd, anc_rows)

    return call(
        kernel,
        [uinv_leaf, uinv_anc, *lefts],
        [live],
        [(rows_here, width), (anc_rows, width), (n_depth, kd, anc_rows)],
        [(n_col, 2, leaf_half, width), (n_col, 2, anc_half, width)] + [(n_col, width, width)] * 2,
        6 * n_col,
        4 * tall * n_col * width * width,
    )


def leaf_upper_panel(linv, top, so_far, live):
    k, wide = top[0][1].shape
    m = linv.shape[0]
    n = len(top)
    before = [] if so_far is None else [so_far]
    scalars = [] if live is None else [live]

    def kernel(*refs):
        live_ref, linv_ref = refs[: len(scalars)], refs[len(scalars)]
        begun = refs[len(scalars) + 1 : len(scalars) + 1 + len(before)]
        blocks = refs[-4 - n : -4]
        out, left, right, sems = refs[-4:]
        copies = []
        for t, ((back, _), ref) in enumerate(zip(top, blocks)):
            at = pl.ds(pl.multiple_of(row_of(back) * k, k), k)
            copies += [(linv_ref.at[:, at], left.at[t]), (ref, right.at[t])]
        started = start_all([*copies, *[(ref, out) for ref in begun]], sems)
        if begun:
            started[-1].wait()
        add_up(out, n, started, 2, lambda t: left[t], lambda t: right[t], not begun)
        if live_ref:
            cols = lax.axis_index("col") * wide + lax.broadcasted_iota(jnp.int32, out.shape, 1)
            out[...] = jnp.where(cols < live_ref[0][0] * NB, out[...], 0.0)

    return call(
        kernel,
        [linv, *before, *[a for _, a in top]],
        scalars,
        [(m, wide)],
        [(n, m, k), (n, k, wide)],
        2 * n + len(before),
        2 * m * n * k * wide,
    )[0]


def add_anc(acc, left, right, n_depth):
    n, kd, wide = right.shape
    anc_rows = left.shape[-1]
    me = lax.axis_index("depth")
    upper = split(right[...].reshape(n * kd, wide))

    def step(ahead, _):
        turned = split(left[lax.rem(me + ahead, n_depth)].reshape(n * kd, anc_rows).T)
        acc[ahead] += dot3(turned, upper)
        return 0

    lax.fori_loop(0, n_depth, step, 0)


def anc_copies(uppers, ups, blocks, left, right, first, n_depth):
    kd = uppers[0][1].shape[0]
    per_half = n_depth // 2
    copies = []
    for t, ((back, _), ref) in enumerate(zip(uppers, ups)):
        copies.append((ref, right.at[t]))
        for which, lower in zip(core_halves(), blocks):
            for j in range(per_half):
                rows = lower.at[row_of(back), pl.ds(first + j * kd, kd)]
                copies.append((rows, left.at[which * per_half + j, t]))
    return copies


def leaf_copies(uppers, ups, blocks, left, right, half_rows):
    copies = []
    for t, ((back, _), ref) in enumerate(zip(uppers, ups)):
        copies.append((ref, right.at[t]))
        for which, lower in zip(core_halves(), blocks):
            copies.append((lower.at[row_of(back), pl.ds(0, half_rows)], left.at[t, which]))
    return copies


def anc_product(lowers, uppers, rows_here, n_depth):
    kd, wide = uppers[0][1].shape
    anc_rows = lowers[0].shape[2]
    n = len(uppers)

    def kernel(*refs):
        blocks, ups = refs[: len(lowers)], refs[len(lowers) : len(lowers) + n]
        acc, left, right, sems = refs[-4:]
        started = start_all(
            anc_copies(uppers, ups, blocks, left, right, rows_here // 2, n_depth), sems
        )
        acc[...] = jnp.zeros_like(acc)
        for c in started:
            c.wait()
        add_anc(acc, left, right, n_depth)

    return call(
        kernel,
        [*lowers, *[a for _, a in uppers]],
        [],
        [(n_depth, anc_rows, wide)],
        [(n_depth, n, kd, anc_rows), (n, kd, wide)],
        (n_depth + 1) * n,
        2 * n_depth * anc_rows * n * kd * wide,
    )[0]


def leaf_product(lowers, uppers, rows_here):
    k, wide = uppers[0][1].shape
    n = len(uppers)
    width = lowers[0].shape[2]

    def kernel(*refs):
        blocks, ups = refs[: len(lowers)], refs[len(lowers) : len(lowers) + n]
        leaf, left, right, sems = refs[-4:]
        started = start_all(leaf_copies(uppers, ups, blocks, left, right, rows_here // 2), sems)
        whole = lambda t: left[t].reshape(rows_here, width)
        add_up(leaf, n, started, 3, whole, lambda t: right[t])

    return call(
        kernel,
        [*lowers, *[a for _, a in uppers]],
        [],
        [(rows_here, wide)],
        [(n, 2, rows_here // 2, width), (n, k, wide)],
        3 * n,
        2 * rows_here * n * k * wide,
    )[0]


def front_parts(lowers, leaf_uppers, anc_uppers, leaf_begun, product, row_map, col_map, rows_here):
    width = lowers[0].shape[2]
    nb = NB
    k, cols_here = leaf_uppers[0][1].shape
    kd = anc_uppers[0][1].shape[0]
    n_depth, owner_rows, wide = product.shape
    per_owner = owner_rows // nb
    half = owner_rows // 2
    n, m = len(leaf_uppers), len(anc_uppers)

    def kernel(rm, cm, prod, begun, *refs):
        blocks, ups = refs[: len(lowers)], refs[len(lowers) : len(lowers) + n]
        anc_ups = refs[len(lowers) + n : len(lowers) + n + m]
        outs = refs[len(lowers) + n + m : -7]
        left, right, anc_left, anc_right, leaf, acc, sems = refs[-7:]
        anc = anc_copies(anc_uppers, anc_ups, blocks, anc_left, anc_right, rows_here // 2, n_depth)
        copies = leaf_copies(leaf_uppers, ups, blocks, left, right, rows_here // 2)
        started = start_all([(begun, leaf), *copies, *anc, (prod, acc)], sems)
        started[0].wait()
        whole = lambda t: left[t].reshape(rows_here, width)
        add_up(leaf, n, started[1:], 3, whole, lambda t: right[t], False)
        for c in started[1 + 3 * n :]:
            c.wait()
        add_anc(acc, anc_left, anc_right, n_depth)
        first_row = lax.axis_index("row") * (n_depth * per_owner)
        first_col = lax.axis_index("col") * (wide // nb)
        me = lax.axis_index("depth")
        for i in range(rows_here // nb):
            at = rm[0, i] - first_row
            ahead = lax.rem(at // per_owner - me + n_depth, n_depth)
            rows = pl.ds(pl.multiple_of(lax.rem(at, per_owner) * nb, nb), nb)
            for j in range(cols_here // nb):
                cols = pl.ds(pl.multiple_of((cm[0, j] - first_col) * nb, nb), nb)
                acc[ahead, rows, cols] += leaf[i * nb : (i + 1) * nb, j * nb : (j + 1) * nb]
        outs[0][...] = acc[0]
        for i, out in enumerate(outs[1:]):
            out[...] = acc[1 + i // 2, pl.ds((i % 2) * half, half)]

    res = call(
        kernel,
        [product, leaf_begun, *lowers, *[a for _, a in leaf_uppers], *[a for _, a in anc_uppers]],
        [row_map, col_map],
        [(owner_rows, wide)] + [(half, wide)] * (2 * (n_depth - 1)),
        [
            (n, 2, rows_here // 2, width),
            (n, k, cols_here),
            (n_depth, m, kd, owner_rows),
            (m, kd, wide),
            (rows_here, cols_here),
            (n_depth, owner_rows, wide),
        ],
        2 + 3 * n + (n_depth + 1) * m,
        2 * rows_here * n * k * cols_here,
    )
    return [res[0]] + [tuple(res[i : i + 2]) for i in range(1, len(res), 2)]


def shards(
    a21_leaf,
    a12_leaf,
    uinv_leaf,
    linv_leaf,
    live,
    row_map,
    col_map,
    a22_anc,
    a21_anc,
    a12_anc,
    uinv_anc,
    linv_anc,
):
    n_row, n_depth = lax.axis_size("row"), lax.axis_size("depth")
    panel_left, panel_top = a21_leaf[0], a12_leaf[0]
    rows_here = panel_left.shape[0]

    anc_top = gather_row(a12_anc, "d")
    leaf_top = gather_row(panel_top, "u")
    linv_got = exchange_depth_rings(split_by_depth(linv_anc, n_row, n_depth))
    halves = lambda leaf, anc: jnp.concatenate(
        [leaf.reshape(2, -1, leaf.shape[1]), anc.reshape(2, -1, anc.shape[1])], axis=1
    )
    lefts = gather_col(halves(panel_left, a21_anc))

    anc_upper = sum(exchange_depth_rings(anc_upper_parts(linv_got, anc_top)))
    leaf_lower, anc_lower, slices = lower_panels(
        lefts, uinv_leaf[0], uinv_anc, live, rows_here, n_depth
    )
    near = 5
    begun = leaf_upper_panel(linv_leaf[0], leaf_top[:near], None, None)
    leaf_upper = leaf_upper_panel(linv_leaf[0], leaf_top[near:], begun, live)

    leaf_uppers = gather_row(leaf_upper, "u")
    anc_uppers = gather_row(anc_upper, "d")
    got_slices = exchange_depth(slices).reshape(a21_anc.shape)
    lowers = gather_col(halves(leaf_lower, got_slices))

    product = anc_product(lowers, anc_uppers[:near], rows_here, n_depth)
    begun = leaf_product(lowers, leaf_uppers[:near], rows_here)
    far = leaf_uppers[near:], anc_uppers[near:]
    parts = front_parts(lowers, *far, begun, product, row_map, col_map, rows_here)
    own, back_top, back_bot, front_top, front_bot = sum_depth(parts)
    half = own.shape[0] // 2
    total_top = own[:half] + back_top + front_top
    total_bot = own[half:] + back_bot + front_bot
    front = a22_anc - jnp.concatenate([total_top, total_bot], axis=0)
    return (leaf_lower[None], leaf_upper[None], anc_lower, anc_upper, front)


def solution(mesh):
    in_specs = (
        P("depth", "row", "col"),
        P("depth", "row", "col"),
        P("depth", None, "col"),
        P("depth", "row", None),
        P("depth"),
        P("depth", "row"),
        P("depth", "col"),
        P(("row", "depth"), "col"),
        P(("row", "depth"), "col"),
        P(("row", "depth"), "col"),
        P(None, "col"),
        P(("row", "depth"), None),
    )
    out_specs = (
        P("depth", "row", "col"),
        P("depth", "row", "col"),
        P(("row", "depth"), "col"),
        P(("row", "depth"), "col"),
        P(("row", "depth"), "col"),
    )
    return jax.shard_map(shards, mesh=mesh, in_specs=in_specs, out_specs=out_specs, check_vma=False)
```

```python
import functools

import jax
import jax.numpy as jnp
from jax import lax
from jax.experimental import pallas as pl
from jax.experimental.pallas import tpu as pltpu
from jax.sharding import PartitionSpec as P

NB = 128
F32 = jnp.float32
BF16 = jnp.bfloat16


def shift(block, axis, step):
    size = lax.axis_size(axis)
    return lax.ppermute(block, axis, [(i, (i + step) % size) for i in range(size)])


def swap_cores(block):
    return lax.ppermute(block, "col", [(i, i ^ 1) for i in range(lax.axis_size("col"))])


def gather_row(block, far):
    steps = lax.axis_size("row") // 2
    got = [(0, block)]
    for way, sign in (("u", 1), ("d", -1)):
        moving = block
        for step in range(1, steps + (way == far)):
            moving = shift(moving, "row", sign)
            got.append((sign * step, moving))
    return got


def gather_col(halves):
    n_col = lax.axis_size("col")
    copies = jnp.broadcast_to(halves, (n_col // 2, *halves.shape)).reshape(n_col, *halves.shape[1:])
    mine = lax.all_to_all(copies, "col", split_axis=0, concat_axis=0, tiled=True)
    return mine, swap_cores(mine)


def exchange_depth(parts):
    return lax.all_to_all(parts, "depth", split_axis=0, concat_axis=0, tiled=True)


def exchange_depth_rings(parts):
    size = len(parts)
    return [parts[0]] + [shift(parts[size - j], "depth", -j) for j in range(1, size)]


def sum_depth(parts):
    own, (one_top, one_bot), (two_top, two_bot), (three_top, three_bot) = parts
    from_back = shift(two_top, "depth", 1)
    from_front = shift(two_bot, "depth", -1)
    back_bot = shift(one_bot, "depth", 1)
    front_top = shift(three_top, "depth", -1)
    back_top = shift(one_top + from_back, "depth", 1)
    front_bot = shift(three_bot + from_front, "depth", -1)
    return own, back_top, back_bot, front_top, front_bot


def split(x):
    high = x.astype(BF16)
    return high, (x - high.astype(F32)).astype(BF16)


def dot3(left, right):
    (lh, ll), (rh, rl) = left, right
    dot = functools.partial(jnp.dot, preferred_element_type=F32)
    return dot(lh, rh) + (dot(lh, rl) + dot(ll, rh))


def start_all(copies, sems):
    started = [pltpu.make_async_copy(src, dst, sems.at[i]) for i, (src, dst) in enumerate(copies)]
    for c in started:
        c.start()
    return started


def copy_all(copies, sems):
    for c in start_all(copies, sems):
        c.wait()


def add_up(out, tiles, landing, sems, left, right):
    out[...] = jnp.zeros_like(out)

    def step(t, _):
        places = landing(t)
        for i, place in enumerate(places):
            pltpu.make_async_copy(place, place, sems.at[t * len(places) + i]).wait()
        out[...] += dot3(split(left(t)), split(right(t)))
        return 0

    lax.fori_loop(0, tiles, step, 0)


def call(kernel, arrays, scalars, outs, scratch, copies, flops):
    specs = [pl.BlockSpec(memory_space=pltpu.SMEM)] * len(scalars)
    specs += [pl.BlockSpec(memory_space=pl.ANY)] * len(arrays)
    return pl.pallas_call(
        kernel,
        in_specs=specs,
        out_specs=[pl.BlockSpec(memory_space=pltpu.VMEM)] * len(outs),
        out_shape=[jax.ShapeDtypeStruct(s, F32) for s in outs],
        scratch_shapes=[
            pltpu.VMEM(s, F32) if isinstance(s[0], int) else pltpu.VMEM(s[0], s[1]) for s in scratch
        ]
        + [pltpu.SemaphoreType.DMA((copies,))],
        compiler_params=pltpu.CompilerParams(vmem_limit_bytes=56 * 2**20),
        cost_estimate=pl.CostEstimate(flops=flops, bytes_accessed=2**20, transcendentals=0),
    )(*scalars, *arrays)


def row_of(back):
    size = lax.axis_size("row")
    return lax.rem(lax.axis_index("row") + (size - back), size)


def core_halves():
    mine = lax.rem(lax.axis_index("col"), 2)
    return mine, 1 - mine


def split_by_depth(linv, n_row, n_depth):
    k, wide = linv.shape
    kd = wide // (n_row * n_depth)

    def kernel(ref, *refs):
        outs, parts = refs[:n_depth], refs[-2]
        for q in range(n_depth):
            cols = [ref[:, (r * n_depth + q) * kd : (r * n_depth + q + 1) * kd] for r in range(n_row)]
            parts[q] = jnp.concatenate(cols, axis=1)
        me = lax.axis_index("depth")
        for j, out in enumerate(outs):
            out[...] = parts[lax.rem(me + j, n_depth)]

    vmem = pl.BlockSpec(memory_space=pltpu.VMEM)
    return pl.pallas_call(
        kernel,
        in_specs=[vmem],
        out_specs=[vmem] * n_depth,
        out_shape=[jax.ShapeDtypeStruct((k, n_row * kd), F32)] * n_depth,
        scratch_shapes=[pltpu.VMEM((n_depth, k, n_row * kd), F32), pltpu.SemaphoreType.DMA((1,))],
    )(linv)


def anc_upper_parts(got_linv, top):
    n_row = lax.axis_size("row")
    k, wide = top[0][1].shape
    n = len(got_linv)
    m, kk = got_linv[0].shape
    tiles = 2
    kt = kk // tiles

    def kernel(*refs):
        linv, blocks, outs = refs[:n], refs[n : n + len(top)], refs[n + len(top) : -4]
        left, right, acc, sems = refs[-4:]
        copies = []
        for j, ref in enumerate(linv):
            for t in range(tiles):
                copies.append((ref.at[:, pl.ds(t * kt, kt)], left.at[t, j]))
        for (back, _), ref in zip(top, blocks):
            copies.append((ref, right.at[row_of(back)]))
        copy_all(copies, sems)

        def step(t, _):
            rows = right[pl.ds(t * (n_row // tiles), n_row // tiles)].reshape(kt, wide)
            got = dot3(split(left[t].reshape(n * m, kt)), split(rows)).reshape(n, m, wide)
            acc[...] = jnp.where(t == 0, got, acc[...] + got)
            return 0

        lax.fori_loop(0, tiles, step, 0)
        for j, out in enumerate(outs):
            out[...] = acc[j]

    return call(
        kernel,
        [*got_linv, *[a for _, a in top]],
        [],
        [(m, wide)] * n,
        [(tiles, n, m, kt), (n_row, k, wide), (n, m, wide)],
        tiles * n + len(top),
        2 * n * m * kk * wide,
    )


def lower_panels(lefts, uinv_leaf, uinv_anc, live, rows_here, n_depth):
    n_col, tall, width = lefts[0].shape
    leaf_half = rows_here // 2
    anc_half = tall - leaf_half
    anc_rows = 2 * anc_half
    kd = width // n_depth

    def kernel(live_ref, ul, ua, mine, other, leaf_out, anc_out, turned, *scratch):
        left_l, left_a, right_l, right_a, sems = scratch
        copies = []
        for t in range(n_col):
            rows = pl.ds(t * width, width)
            copies += [(ul.at[rows], right_l.at[t]), (ua.at[rows], right_a.at[t])]
            for which, ref in zip(core_halves(), (mine, other)):
                copies += [
                    (ref.at[t, pl.ds(0, leaf_half)], left_l.at[t, which]),
                    (ref.at[t, pl.ds(leaf_half, anc_half)], left_a.at[t, which]),
                ]
        start_all(copies, sems)
        anc = lambda t: left_a[t].reshape(anc_rows, width)
        leaf = lambda t: left_l[t].reshape(rows_here, width)
        landing = lambda t: (
            right_l.at[t],
            right_a.at[t],
            left_l.at[t, 0],
            left_a.at[t, 0],
            left_l.at[t, 1],
            left_a.at[t, 1],
        )
        add_up(anc_out, n_col, landing, sems, anc, lambda t: right_a[t])
        add_up(leaf_out, n_col, lambda t: (), sems, leaf, lambda t: right_l[t])
        rows = lax.axis_index("row") * rows_here + lax.broadcasted_iota(jnp.int32, leaf_out.shape, 0)
        leaf_out[...] = jnp.where(rows < live_ref[0] * NB, leaf_out[...], 0.0)
        turned[...] = anc_out[...].T.reshape(n_depth, kd, anc_rows)

    return call(
        kernel,
        [uinv_leaf, uinv_anc, *lefts],
        [live],
        [(rows_here, width), (anc_rows, width), (n_depth, kd, anc_rows)],
        [(n_col, 2, leaf_half, width), (n_col, 2, anc_half, width)] + [(n_col, width, width)] * 2,
        6 * n_col,
        4 * tall * n_col * width * width,
    )


def leaf_upper_panel(linv, top, live):
    n_row = lax.axis_size("row")
    k, wide = top[0][1].shape
    m = linv.shape[0]

    def kernel(live_ref, linv_ref, *refs):
        blocks = refs[: len(top)]
        out, left, right, sems = refs[len(top) :]
        copies = []
        for t, ((back, _), ref) in enumerate(zip(top, blocks)):
            at = pl.ds(pl.multiple_of(row_of(back) * k, k), k)
            copies += [(linv_ref.at[:, at], left.at[t]), (ref, right.at[t])]
        start_all(copies, sems)
        landing = lambda t: (left.at[t], right.at[t])
        add_up(out, n_row, landing, sems, lambda t: left[t], lambda t: right[t])
        cols = lax.axis_index("col") * wide + lax.broadcasted_iota(jnp.int32, out.shape, 1)
        out[...] = jnp.where(cols < live_ref[0] * NB, out[...], 0.0)

    return call(
        kernel,
        [linv, *[a for _, a in top]],
        [live],
        [(m, wide)],
        [(n_row, m, k), (n_row, k, wide)],
        2 * n_row,
        2 * m * n_row * k * wide,
    )[0]


def anc_product(lowers, uppers, rows_here, n_depth):
    n_row = lax.axis_size("row")
    kd, wide = uppers[0][1].shape
    n_col, tall, anc_rows = lowers[0].shape
    first, per_half = rows_here // 2, n_depth // 2
    assert tall == first + per_half * kd
    tiles = 2
    kt = n_row * kd // tiles

    def kernel(*refs):
        blocks, ups = refs[: len(lowers)], refs[len(lowers) : len(lowers) + len(uppers)]
        acc, left, right, high, low, sems = refs[-6:]
        copies = []
        for which, ref in zip(core_halves(), blocks):
            for j in range(per_half):
                rows = ref.at[:, pl.ds(first + j * kd, kd)]
                copies.append((rows, left.at[which * per_half + j]))
        for (back, _), ref in zip(uppers, ups):
            copies.append((ref, right.at[row_of(back)]))
        copy_all(copies, sems)
        for t in range(tiles):
            n = n_row // tiles
            high[t], low[t] = split(right[t * n : (t + 1) * n].reshape(kt, wide))

        me = lax.axis_index("depth")

        def step(i, _):
            t = lax.rem(i, tiles)
            j = lax.rem(me + i // tiles, n_depth)
            turned = split(left[j, pl.ds(t * (n_col // tiles), n_col // tiles)].reshape(kt, anc_rows).T)
            got = dot3(turned, (high[t], low[t]))
            ahead = i // tiles
            acc[ahead] = jnp.where(t == 0, got, acc[ahead] + got)
            return 0

        lax.fori_loop(0, n_depth * tiles, step, 0)

    return call(
        kernel,
        [*lowers, *[a for _, a in uppers]],
        [],
        [(n_depth, anc_rows, wide)],
        [
            (n_depth, n_col, kd, anc_rows),
            (n_row, kd, wide),
            ((tiles, kt, wide), BF16),
            ((tiles, kt, wide), BF16),
        ],
        n_depth + len(uppers),
        2 * n_depth * anc_rows * n_row * kd * wide,
    )[0]


def front_parts(lowers, uppers, product, row_map, col_map, rows_here):
    n_row = lax.axis_size("row")
    n_col, _, width = lowers[0].shape
    half_rows = rows_here // 2
    nb = NB
    k, cols_here = uppers[0][1].shape
    n_depth, owner_rows, wide = product.shape
    per_owner = owner_rows // nb
    half = owner_rows // 2

    def kernel(rm, cm, prod, *refs):
        blocks, ups = refs[: len(lowers)], refs[len(lowers) : len(lowers) + len(uppers)]
        outs = refs[len(lowers) + len(uppers) : -5]
        left, right, leaf, acc, sems = refs[-5:]
        copies = []
        for t, ((back, _), ref) in enumerate(zip(uppers, ups)):
            row = row_of(back)
            copies.append((ref, right.at[t]))
            for which, lower in zip(core_halves(), blocks):
                copies.append((lower.at[row, pl.ds(0, half_rows)], left.at[t, which]))
        started = start_all([*copies, (prod, acc)], sems)
        whole = lambda t: left[t].reshape(rows_here, width)
        landing = lambda t: (right.at[t], left.at[t, 0], left.at[t, 1])
        add_up(leaf, n_row, landing, sems, whole, lambda t: right[t])
        started[-1].wait()
        first_row = lax.axis_index("row") * (n_depth * per_owner)
        first_col = lax.axis_index("col") * (wide // nb)
        me = lax.axis_index("depth")
        for i in range(rows_here // nb):
            at = rm[0, i] - first_row
            ahead = lax.rem(at // per_owner - me + n_depth, n_depth)
            rows = pl.ds(pl.multiple_of(lax.rem(at, per_owner) * nb, nb), nb)
            for j in range(cols_here // nb):
                cols = pl.ds(pl.multiple_of((cm[0, j] - first_col) * nb, nb), nb)
                acc[ahead, rows, cols] += leaf[i * nb : (i + 1) * nb, j * nb : (j + 1) * nb]
        outs[0][...] = acc[0]
        for i, out in enumerate(outs[1:]):
            out[...] = acc[1 + i // 2, pl.ds((i % 2) * half, half)]

    res = call(
        kernel,
        [product, *lowers, *[a for _, a in uppers]],
        [row_map, col_map],
        [(owner_rows, wide)] + [(half, wide)] * (2 * (n_depth - 1)),
        [
            (n_col, 2, half_rows, width),
            (n_row, k, cols_here),
            (rows_here, cols_here),
            (n_depth, owner_rows, wide),
        ],
        3 * n_row + 1,
        2 * rows_here * n_row * k * cols_here,
    )
    return [res[0]] + [tuple(res[i : i + 2]) for i in range(1, len(res), 2)]


def shards(
    a21_leaf,
    a12_leaf,
    uinv_leaf,
    linv_leaf,
    live,
    row_map,
    col_map,
    a22_anc,
    a21_anc,
    a12_anc,
    uinv_anc,
    linv_anc,
):
    n_row, n_depth = lax.axis_size("row"), lax.axis_size("depth")
    panel_left, panel_top = a21_leaf[0], a12_leaf[0]
    rows_here = panel_left.shape[0]

    anc_top = gather_row(a12_anc, "d")
    leaf_top = gather_row(panel_top, "u")
    linv_got = exchange_depth_rings(split_by_depth(linv_anc, n_row, n_depth))
    halves = lambda leaf, anc: jnp.concatenate(
        [leaf.reshape(2, -1, leaf.shape[1]), anc.reshape(2, -1, anc.shape[1])], axis=1
    )
    lefts = gather_col(halves(panel_left, a21_anc))

    anc_upper = sum(exchange_depth_rings(anc_upper_parts(linv_got, anc_top)))
    leaf_lower, anc_lower, slices = lower_panels(
        lefts, uinv_leaf[0], uinv_anc, live, rows_here, n_depth
    )
    leaf_upper = leaf_upper_panel(linv_leaf[0], leaf_top, live)

    leaf_uppers = gather_row(leaf_upper, "u")
    anc_uppers = gather_row(anc_upper, "d")
    got_slices = exchange_depth(slices).reshape(a21_anc.shape)
    lowers = gather_col(halves(leaf_lower, got_slices))

    product = anc_product(lowers, anc_uppers, rows_here, n_depth)
    parts = front_parts(lowers, leaf_uppers, product, row_map, col_map, rows_here)
    own, back_top, back_bot, front_top, front_bot = sum_depth(parts)
    half = own.shape[0] // 2
    total_top = own[:half] + back_top + front_top
    total_bot = own[half:] + back_bot + front_bot
    front = a22_anc - jnp.concatenate([total_top, total_bot], axis=0)
    return (leaf_lower[None], leaf_upper[None], anc_lower, anc_upper, front)


def solution(mesh):
    in_specs = (
        P("depth", "row", "col"),
        P("depth", "row", "col"),
        P("depth", None, "col"),
        P("depth", "row", None),
        P("depth"),
        P("depth", "row"),
        P("depth", "col"),
        P(("row", "depth"), "col"),
        P(("row", "depth"), "col"),
        P(("row", "depth"), "col"),
        P(None, "col"),
        P(("row", "depth"), None),
    )
    out_specs = (
        P("depth", "row", "col"),
        P("depth", "row", "col"),
        P(("row", "depth"), "col"),
        P(("row", "depth"), "col"),
        P(("row", "depth"), "col"),
    )
    return jax.shard_map(shards, mesh=mesh, in_specs=in_specs, out_specs=out_specs, check_vma=False)
```

```python
import functools

import jax
import jax.numpy as jnp
from jax import lax
from jax.experimental import pallas as pl
from jax.experimental.pallas import tpu as pltpu
from jax.sharding import PartitionSpec as P

NB = 128
F32 = jnp.float32
BF16 = jnp.bfloat16


def shift(block, axis, step):
    size = lax.axis_size(axis)
    return lax.ppermute(block, axis, [(i, (i + step) % size) for i in range(size)])


def swap_cores(block):
    return lax.ppermute(block, "col", [(i, i ^ 1) for i in range(lax.axis_size("col"))])


def gather_row(block, far):
    steps = lax.axis_size("row") // 2
    got = [(0, block)]
    for way, sign in (("u", 1), ("d", -1)):
        moving = block
        for step in range(1, steps + (way == far)):
            moving = shift(moving, "row", sign)
            got.append((sign * step, moving))
    return got


def gather_col(halves):
    n_col = lax.axis_size("col")
    copies = jnp.broadcast_to(halves, (n_col // 2, *halves.shape)).reshape(n_col, *halves.shape[1:])
    mine = lax.all_to_all(copies, "col", split_axis=0, concat_axis=0, tiled=True)
    return mine, swap_cores(mine)


def exchange_depth(parts):
    return lax.all_to_all(parts, "depth", split_axis=0, concat_axis=0, tiled=True)


def exchange_depth_rings(parts):
    size = len(parts)
    return [parts[0]] + [shift(parts[size - j], "depth", -j) for j in range(1, size)]


def sum_depth(parts):
    own, (one_top, one_bot), (two_top, two_bot), (three_top, three_bot) = parts
    from_back = shift(two_top, "depth", 1)
    from_front = shift(two_bot, "depth", -1)
    back_bot = shift(one_bot, "depth", 1)
    front_top = shift(three_top, "depth", -1)
    back_top = shift(one_top + from_back, "depth", 1)
    front_bot = shift(three_bot + from_front, "depth", -1)
    return own, back_top, back_bot, front_top, front_bot


def split(x):
    high = x.astype(BF16)
    return high, (x - high.astype(F32)).astype(BF16)


def dot3(left, right):
    (lh, ll), (rh, rl) = left, right
    dot = functools.partial(jnp.dot, preferred_element_type=F32)
    return dot(lh, rh) + (dot(lh, rl) + dot(ll, rh))


def start_all(copies, sems):
    started = [pltpu.make_async_copy(src, dst, sems.at[i]) for i, (src, dst) in enumerate(copies)]
    for c in started:
        c.start()
    return started


def copy_all(copies, sems):
    for c in start_all(copies, sems):
        c.wait()


def add_up(out, tiles, started, per_tile, left, right):
    for t in range(tiles):
        for c in started[t * per_tile : (t + 1) * per_tile]:
            c.wait()
        got = dot3(split(left(t)), split(right(t)))
        out[...] = got if t == 0 else out[...] + got


def call(kernel, arrays, scalars, outs, scratch, copies, flops):
    specs = [pl.BlockSpec(memory_space=pltpu.SMEM)] * len(scalars)
    specs += [pl.BlockSpec(memory_space=pl.ANY)] * len(arrays)
    return pl.pallas_call(
        kernel,
        in_specs=specs,
        out_specs=[pl.BlockSpec(memory_space=pltpu.VMEM)] * len(outs),
        out_shape=[jax.ShapeDtypeStruct(s, F32) for s in outs],
        scratch_shapes=[
            pltpu.VMEM(s, F32) if isinstance(s[0], int) else pltpu.VMEM(s[0], s[1]) for s in scratch
        ]
        + [pltpu.SemaphoreType.DMA((copies,))],
        compiler_params=pltpu.CompilerParams(vmem_limit_bytes=56 * 2**20),
        cost_estimate=pl.CostEstimate(flops=flops, bytes_accessed=2**20, transcendentals=0),
    )(*scalars, *arrays)


def row_of(back):
    size = lax.axis_size("row")
    return lax.rem(lax.axis_index("row") + (size - back), size)


def core_halves():
    mine = lax.rem(lax.axis_index("col"), 2)
    return mine, 1 - mine


def split_by_depth(linv, n_row, n_depth):
    k, wide = linv.shape
    kd = wide // (n_row * n_depth)

    def kernel(ref, *refs):
        outs, parts = refs[:n_depth], refs[-2]
        for q in range(n_depth):
            cols = [ref[:, (r * n_depth + q) * kd : (r * n_depth + q + 1) * kd] for r in range(n_row)]
            parts[q] = jnp.concatenate(cols, axis=1)
        me = lax.axis_index("depth")
        for j, out in enumerate(outs):
            out[...] = parts[lax.rem(me + j, n_depth)]

    vmem = pl.BlockSpec(memory_space=pltpu.VMEM)
    return pl.pallas_call(
        kernel,
        in_specs=[vmem],
        out_specs=[vmem] * n_depth,
        out_shape=[jax.ShapeDtypeStruct((k, n_row * kd), F32)] * n_depth,
        scratch_shapes=[pltpu.VMEM((n_depth, k, n_row * kd), F32), pltpu.SemaphoreType.DMA((1,))],
    )(linv)


def anc_upper_parts(got_linv, top):
    n_row = lax.axis_size("row")
    k, wide = top[0][1].shape
    n = len(got_linv)
    m, kk = got_linv[0].shape
    tiles = 2
    kt = kk // tiles

    def kernel(*refs):
        linv, blocks, outs = refs[:n], refs[n : n + len(top)], refs[n + len(top) : -4]
        left, right, acc, sems = refs[-4:]
        copies = []
        for j, ref in enumerate(linv):
            for t in range(tiles):
                copies.append((ref.at[:, pl.ds(t * kt, kt)], left.at[t, j]))
        for (back, _), ref in zip(top, blocks):
            copies.append((ref, right.at[row_of(back)]))
        copy_all(copies, sems)

        def step(t, _):
            rows = right[pl.ds(t * (n_row // tiles), n_row // tiles)].reshape(kt, wide)
            got = dot3(split(left[t].reshape(n * m, kt)), split(rows)).reshape(n, m, wide)
            acc[...] = jnp.where(t == 0, got, acc[...] + got)
            return 0

        lax.fori_loop(0, tiles, step, 0)
        for j, out in enumerate(outs):
            out[...] = acc[j]

    return call(
        kernel,
        [*got_linv, *[a for _, a in top]],
        [],
        [(m, wide)] * n,
        [(tiles, n, m, kt), (n_row, k, wide), (n, m, wide)],
        tiles * n + len(top),
        2 * n * m * kk * wide,
    )


def lower_panels(lefts, uinv_leaf, uinv_anc, live, rows_here, n_depth):
    n_col, tall, width = lefts[0].shape
    leaf_half = rows_here // 2
    anc_half = tall - leaf_half
    anc_rows = 2 * anc_half
    kd = width // n_depth

    def kernel(live_ref, ul, ua, mine, other, leaf_out, anc_out, turned, *scratch):
        left_l, left_a, right_l, right_a, sems = scratch
        copies = []
        for t in range(n_col):
            rows = pl.ds(t * width, width)
            copies += [(ul.at[rows], right_l.at[t]), (ua.at[rows], right_a.at[t])]
            for which, ref in zip(core_halves(), (mine, other)):
                copies += [
                    (ref.at[t, pl.ds(0, leaf_half)], left_l.at[t, which]),
                    (ref.at[t, pl.ds(leaf_half, anc_half)], left_a.at[t, which]),
                ]
        started = start_all(copies, sems)
        anc = lambda t: left_a[t].reshape(anc_rows, width)
        leaf = lambda t: left_l[t].reshape(rows_here, width)
        add_up(anc_out, n_col, started, 6, anc, lambda t: right_a[t])
        add_up(leaf_out, n_col, started, 0, leaf, lambda t: right_l[t])
        rows = lax.axis_index("row") * rows_here + lax.broadcasted_iota(jnp.int32, leaf_out.shape, 0)
        leaf_out[...] = jnp.where(rows < live_ref[0] * NB, leaf_out[...], 0.0)
        turned[...] = anc_out[...].T.reshape(n_depth, kd, anc_rows)

    return call(
        kernel,
        [uinv_leaf, uinv_anc, *lefts],
        [live],
        [(rows_here, width), (anc_rows, width), (n_depth, kd, anc_rows)],
        [(n_col, 2, leaf_half, width), (n_col, 2, anc_half, width)] + [(n_col, width, width)] * 2,
        6 * n_col,
        4 * tall * n_col * width * width,
    )


def leaf_upper_panel(linv, top, live):
    n_row = lax.axis_size("row")
    k, wide = top[0][1].shape
    m = linv.shape[0]

    def kernel(live_ref, linv_ref, *refs):
        blocks = refs[: len(top)]
        out, left, right, sems = refs[len(top) :]
        copies = []
        for t, ((back, _), ref) in enumerate(zip(top, blocks)):
            at = pl.ds(pl.multiple_of(row_of(back) * k, k), k)
            copies += [(linv_ref.at[:, at], left.at[t]), (ref, right.at[t])]
        started = start_all(copies, sems)
        add_up(out, n_row, started, 2, lambda t: left[t], lambda t: right[t])
        cols = lax.axis_index("col") * wide + lax.broadcasted_iota(jnp.int32, out.shape, 1)
        out[...] = jnp.where(cols < live_ref[0] * NB, out[...], 0.0)

    return call(
        kernel,
        [linv, *[a for _, a in top]],
        [live],
        [(m, wide)],
        [(n_row, m, k), (n_row, k, wide)],
        2 * n_row,
        2 * m * n_row * k * wide,
    )[0]


def anc_product(lowers, uppers, rows_here, n_depth):
    n_row = lax.axis_size("row")
    kd, wide = uppers[0][1].shape
    n_col, tall, anc_rows = lowers[0].shape
    first, per_half = rows_here // 2, n_depth // 2
    assert tall == first + per_half * kd
    tiles = 2
    kt = n_row * kd // tiles

    def kernel(*refs):
        blocks, ups = refs[: len(lowers)], refs[len(lowers) : len(lowers) + len(uppers)]
        acc, left, right, high, low, sems = refs[-6:]
        copies = []
        for which, ref in zip(core_halves(), blocks):
            for j in range(per_half):
                rows = ref.at[:, pl.ds(first + j * kd, kd)]
                copies.append((rows, left.at[which * per_half + j]))
        for (back, _), ref in zip(uppers, ups):
            copies.append((ref, right.at[row_of(back)]))
        copy_all(copies, sems)
        for t in range(tiles):
            n = n_row // tiles
            high[t], low[t] = split(right[t * n : (t + 1) * n].reshape(kt, wide))

        me = lax.axis_index("depth")

        def step(i, _):
            t = lax.rem(i, tiles)
            j = lax.rem(me + i // tiles, n_depth)
            turned = split(left[j, pl.ds(t * (n_col // tiles), n_col // tiles)].reshape(kt, anc_rows).T)
            got = dot3(turned, (high[t], low[t]))
            ahead = i // tiles
            acc[ahead] = jnp.where(t == 0, got, acc[ahead] + got)
            return 0

        lax.fori_loop(0, n_depth * tiles, step, 0)

    return call(
        kernel,
        [*lowers, *[a for _, a in uppers]],
        [],
        [(n_depth, anc_rows, wide)],
        [
            (n_depth, n_col, kd, anc_rows),
            (n_row, kd, wide),
            ((tiles, kt, wide), BF16),
            ((tiles, kt, wide), BF16),
        ],
        n_depth + len(uppers),
        2 * n_depth * anc_rows * n_row * kd * wide,
    )[0]


def front_parts(lowers, uppers, product, row_map, col_map, rows_here):
    n_row = lax.axis_size("row")
    n_col, _, width = lowers[0].shape
    half_rows = rows_here // 2
    nb = NB
    k, cols_here = uppers[0][1].shape
    n_depth, owner_rows, wide = product.shape
    per_owner = owner_rows // nb
    half = owner_rows // 2

    def kernel(rm, cm, prod, *refs):
        blocks, ups = refs[: len(lowers)], refs[len(lowers) : len(lowers) + len(uppers)]
        outs = refs[len(lowers) + len(uppers) : -5]
        left, right, leaf, acc, sems = refs[-5:]
        copies = []
        for t, ((back, _), ref) in enumerate(zip(uppers, ups)):
            row = row_of(back)
            copies.append((ref, right.at[t]))
            for which, lower in zip(core_halves(), blocks):
                copies.append((lower.at[row, pl.ds(0, half_rows)], left.at[t, which]))
        started = start_all([*copies, (prod, acc)], sems)
        whole = lambda t: left[t].reshape(rows_here, width)
        add_up(leaf, n_row, started, 3, whole, lambda t: right[t])
        started[-1].wait()
        first_row = lax.axis_index("row") * (n_depth * per_owner)
        first_col = lax.axis_index("col") * (wide // nb)
        me = lax.axis_index("depth")
        for i in range(rows_here // nb):
            at = rm[0, i] - first_row
            ahead = lax.rem(at // per_owner - me + n_depth, n_depth)
            rows = pl.ds(pl.multiple_of(lax.rem(at, per_owner) * nb, nb), nb)
            for j in range(cols_here // nb):
                cols = pl.ds(pl.multiple_of((cm[0, j] - first_col) * nb, nb), nb)
                acc[ahead, rows, cols] += leaf[i * nb : (i + 1) * nb, j * nb : (j + 1) * nb]
        outs[0][...] = acc[0]
        for i, out in enumerate(outs[1:]):
            out[...] = acc[1 + i // 2, pl.ds((i % 2) * half, half)]

    res = call(
        kernel,
        [product, *lowers, *[a for _, a in uppers]],
        [row_map, col_map],
        [(owner_rows, wide)] + [(half, wide)] * (2 * (n_depth - 1)),
        [
            (n_col, 2, half_rows, width),
            (n_row, k, cols_here),
            (rows_here, cols_here),
            (n_depth, owner_rows, wide),
        ],
        3 * n_row + 1,
        2 * rows_here * n_row * k * cols_here,
    )
    return [res[0]] + [tuple(res[i : i + 2]) for i in range(1, len(res), 2)]


def shards(
    a21_leaf,
    a12_leaf,
    uinv_leaf,
    linv_leaf,
    live,
    row_map,
    col_map,
    a22_anc,
    a21_anc,
    a12_anc,
    uinv_anc,
    linv_anc,
):
    n_row, n_depth = lax.axis_size("row"), lax.axis_size("depth")
    panel_left, panel_top = a21_leaf[0], a12_leaf[0]
    rows_here = panel_left.shape[0]

    anc_top = gather_row(a12_anc, "d")
    leaf_top = gather_row(panel_top, "u")
    linv_got = exchange_depth_rings(split_by_depth(linv_anc, n_row, n_depth))
    halves = lambda leaf, anc: jnp.concatenate(
        [leaf.reshape(2, -1, leaf.shape[1]), anc.reshape(2, -1, anc.shape[1])], axis=1
    )
    lefts = gather_col(halves(panel_left, a21_anc))

    anc_upper = sum(exchange_depth_rings(anc_upper_parts(linv_got, anc_top)))
    leaf_lower, anc_lower, slices = lower_panels(
        lefts, uinv_leaf[0], uinv_anc, live, rows_here, n_depth
    )
    leaf_upper = leaf_upper_panel(linv_leaf[0], leaf_top, live)

    leaf_uppers = gather_row(leaf_upper, "u")
    anc_uppers = gather_row(anc_upper, "d")
    got_slices = exchange_depth(slices).reshape(a21_anc.shape)
    lowers = gather_col(halves(leaf_lower, got_slices))

    product = anc_product(lowers, anc_uppers, rows_here, n_depth)
    parts = front_parts(lowers, leaf_uppers, product, row_map, col_map, rows_here)
    own, back_top, back_bot, front_top, front_bot = sum_depth(parts)
    half = own.shape[0] // 2
    total_top = own[:half] + back_top + front_top
    total_bot = own[half:] + back_bot + front_bot
    front = a22_anc - jnp.concatenate([total_top, total_bot], axis=0)
    return (leaf_lower[None], leaf_upper[None], anc_lower, anc_upper, front)


def solution(mesh):
    in_specs = (
        P("depth", "row", "col"),
        P("depth", "row", "col"),
        P("depth", None, "col"),
        P("depth", "row", None),
        P("depth"),
        P("depth", "row"),
        P("depth", "col"),
        P(("row", "depth"), "col"),
        P(("row", "depth"), "col"),
        P(("row", "depth"), "col"),
        P(None, "col"),
        P(("row", "depth"), None),
    )
    out_specs = (
        P("depth", "row", "col"),
        P("depth", "row", "col"),
        P(("row", "depth"), "col"),
        P(("row", "depth"), "col"),
        P(("row", "depth"), "col"),
    )
    return jax.shard_map(shards, mesh=mesh, in_specs=in_specs, out_specs=out_specs, check_vma=False)
```
